32 devices in a mesh: row: 8 (over z, x), col: 4 (over y, core).
Axes of the slice: x: 2, y: 2, z: 4, core: 2. Of those that a mesh axis runs over, the one named last changes fastest.
Arguments:
- matrix: float32 [5, 8, 10, 4, 128, 128], P(None, 'row', None, 'col'), may hold values from 0 to 2.5, as said below
- flags: int32 [5, 8, 10, 4], P(None, 'row', None, 'col'), may hold values from 0 to 1, as said below
Outputs:
- factor: float32 [5, 8, 10, 4, 128, 128], P(None, 'row', None, 'col')
The draws below stay inside these ranges and needn't reach their ends.
Inputs may be any that keep to these rules, and one draw needn't show every extreme that they name: `matrix`: symmetric positive definite, of order 40*128, diagonal at least 1.5. `flags`: 0 marks a float32 tile, 1 a bfloat16 tile; every diagonal tile is 0.
All inputs are finite; a program needn't handle non-finite values.
Results may differ from the reference program's by a relative error of at most 0.0005.
The reference program's roundings to bfloat16 on the way count: a program that leaves them out, or rounds other values in their place, can miss the bound.
Values sent between devices are 32-bit elements; how exact they have to be, the bound alone decides.
No kernel may reach another device: no remote copies, remote signals or barrier semaphores. Data moves between devices by JAX's collectives and lax.ppermute only.
A program may use at most 128 MiB of HBM per device.

```python
import jax
import jax.numpy as jnp
from jax import lax

B = 128
PT = 4
TR_DEV = 5
NT = 40
TC_DEV = 10


def draw_matrix(key, part):
    count = NT * B
    points = jax.random.uniform(jax.random.fold_in(key, 11), (count, 2), jnp.float32)
    order = jnp.argsort(points[:, 0])
    points = points[order]
    reach = 0.6
    nugget = 0.5
    delta_x = points[:, 0][:, None] - points[:, 0][None, :]
    delta_y = points[:, 1][:, None] - points[:, 1][None, :]
    dist = jnp.sqrt(delta_x * delta_x + delta_y * delta_y)
    cov = jnp.exp(-dist / reach) + nugget * jnp.eye(count, dtype=jnp.float32)
    tiled = cov.reshape(NT, B, NT, B).transpose(0, 2, 1, 3)
    return tiled.reshape(TR_DEV, NT // TR_DEV, TC_DEV, NT // TC_DEV, B, B)


def draw_flags(key, part):
    tile_ids = jnp.arange(NT, dtype=jnp.int32)
    spacing = jnp.abs(tile_ids[:, None] - tile_ids[None, :])
    band = jax.random.randint(jax.random.fold_in(key, 5), (), 2, 6)
    flips = jax.random.randint(jax.random.fold_in(key, 7), (NT, NT), 0, 4)
    far_mark = (flips != 0).astype(jnp.int32)
    near_mark = (flips == 0).astype(jnp.int32)
    marks = jnp.where(spacing == 0, 0, jnp.where(spacing >= band, far_mark, near_mark))
    return marks.astype(jnp.int32).reshape(TR_DEV, NT // TR_DEV, TC_DEV, NT // TC_DEV)


def setup_inputs(seed: int = 0) -> dict:
    key_list = jax.random.split(jax.random.key(seed), 3)
    matrix = draw_matrix(jax.random.fold_in(key_list[2], 71), 0)
    flags = draw_flags(jax.random.fold_in(key_list[2], 71), 0)
    return {"matrix": matrix, "flags": flags}


def storage_round(values):
    narrow = lax.optimization_barrier(values.astype(jnp.bfloat16))
    return narrow.astype(jnp.float32)

def reference(matrix, flags):
    width = PT * B
    tiles = matrix.reshape(NT, NT, B, B)
    marks = flags.reshape(NT, NT)
    work = jnp.where((marks == 1)[:, :, None, None], storage_round(tiles), tiles)
    tile_ids = jnp.arange(NT, dtype=jnp.int32)
    for step in range(2):
        start = step * PT
        rows = work[:, start:start + PT].transpose(0, 2, 1, 3).reshape(NT, B, width)
        dense = rows[start:start + PT].reshape(width, width)
        sym = jnp.tril(dense) + jnp.tril(dense, -1).T
        lower_block = jnp.linalg.cholesky(sym)
        flat = rows.reshape(NT * B, width)
        solved = jax.scipy.linalg.solve_triangular(lower_block, flat.T, lower=True).T.reshape(NT, B, width)
        solved = solved.at[start:start + PT].set(lower_block.reshape(PT, B, width))
        rounded = storage_round(solved)

        def row_update(args):
            tile_row, mark_row, index = args
            exact = jnp.einsum('ik,cjk->cij', solved[index], solved, precision=lax.Precision.HIGHEST)
            coarse = jnp.einsum('ik,cjk->cij', rounded[index], rounded, precision=lax.Precision.HIGHEST)
            live = (index >= tile_ids) & (tile_ids >= start + PT)
            updated = jnp.where((mark_row == 1)[:, None, None], tile_row - coarse, tile_row - exact)
            return jnp.where(live[:, None, None], updated, tile_row)
        work = lax.map(row_update, (work, marks, tile_ids))
        new_cols = solved.reshape(NT, B, PT, B).transpose(0, 2, 1, 3)
        keep = (tile_ids >= start)[:, None, None, None]
        work = work.at[:, start:start + PT].set(jnp.where(keep, new_cols, work[:, start:start + PT]))
    final = jnp.where((marks == 1)[:, :, None, None], storage_round(work), work)
    upper = tile_ids[:, None] < tile_ids[None, :]
    final = jnp.where(upper[:, :, None, None], jnp.float32(0.0), final)
    return final.reshape(TR_DEV, NT // TR_DEV, TC_DEV, NT // TC_DEV, B, B)
```

```python
import functools

import jax
import jax.numpy as jnp
from jax import lax
from jax.experimental import pallas as pl
from jax.experimental.pallas import tpu as pltpu
from jax.sharding import PartitionSpec as P

PT = 4
STEPS = 2
PAD = 8
WIDTH = 16
HIGHEST = lax.Precision.HIGHEST


def storage_round(values):
    narrow = lax.optimization_barrier(values.astype(jnp.bfloat16))
    return narrow.astype(jnp.float32)


def exact_dot(left, right, left_dim=1, right_dim=0):
    return lax.dot_general(
        left,
        right,
        (((left_dim,), (right_dim,)), ((), ())),
        precision=HIGHEST,
        preferred_element_type=jnp.float32,
    )


def coarse_dot(left, right, left_dim=1, right_dim=0):
    return lax.dot_general(
        left.astype(jnp.bfloat16),
        right.astype(jnp.bfloat16),
        (((left_dim,), (right_dim,)), ((), ())),
        preferred_element_type=jnp.float32,
    )


def invert_tile(a_ref, b_ref, q_ref, out_ref):
    tile = a_ref.shape[0]
    ids = lax.broadcasted_iota(jnp.int32, (WIDTH, tile), 0)
    row_ids = lax.broadcasted_iota(jnp.int32, (tile, tile), 0)
    lane_ids = lax.broadcasted_iota(jnp.int32, (tile, tile), 1)
    b_ref[...] = (row_ids == lane_ids).astype(jnp.float32)
    q_ref[...] = jnp.zeros(q_ref.shape, jnp.float32)
    for low in range(0, tile, WIDTH):
        high = low + WIDTH
        rows = a_ref[low:high, :]
        extra = b_ref[low:high, :]
        columns = [
            jnp.broadcast_to(rows[:, low + j : low + j + 1], (WIDTH, tile)) for j in range(WIDTH)
        ]
        scale = jnp.zeros((WIDTH, tile), jnp.float32)
        for k in range(WIDTH):
            root = lax.rsqrt(columns[k][k : k + 1, :])
            inverse = root * root
            pivot_extra = extra[k : k + 1, :]
            out_ref[low + k : low + k + 1, :] = pivot_extra * root
            factor = jnp.where(ids == k, 0.0, columns[k] * inverse)
            for j in range(k + 1, WIDTH):
                columns[j] = columns[j] - factor * columns[j][k : k + 1, :]
            rows = rows - factor * rows[k : k + 1, :]
            extra = extra - factor * pivot_extra
            scale = jnp.where(ids == k, inverse, scale)
        if high < tile:
            q_ref[low:high, :tile] = rows * scale
            q_ref[low:high, tile:] = extra * scale
            below = a_ref[high:, :]
            update = exact_dot(below, q_ref[...])
            a_ref[high:, :] = below - update[:, :tile]
            b_ref[high:, :] = b_ref[high:, :] - update[:, tile:]
            q_ref[low:high, :] = jnp.zeros((WIDTH, 2 * tile), jnp.float32)


def invert_kernel(dense_ref, out_ref, work, extra, a_ref, b_ref, q_ref, l_ref):
    tile = a_ref.shape[0]
    size = work.shape[0]
    work[...] = dense_ref[...]
    extra[...] = jnp.zeros(extra.shape, jnp.float32)
    out_ref[...] = jnp.zeros(out_ref.shape, jnp.float32)
    for low in range(0, size, tile):
        high = low + tile
        a_ref[...] = work[low:high, low:high]
        invert_tile(a_ref, b_ref, q_ref, l_ref)
        lower = l_ref[...]
        out_ref[low:high, low:high] = lower
        if low:
            out_ref[low:high, :low] = exact_dot(lower, extra[low:high, :low])
        if high < size:
            inverse = exact_dot(lower, lower, 0, 0)
            below = work[high:, low:high]
            work[high:, high:] = work[high:, high:] - exact_dot(
                below, exact_dot(inverse, work[low:high, high:])
            )
            if low:
                extra[high:, :low] = extra[high:, :low] - exact_dot(
                    below, exact_dot(inverse, extra[low:high, :low])
                )
            extra[high:, low:high] = -exact_dot(below, inverse)


def inverse_factor(dense, tile):
    size = dense.shape[0]
    f32 = jnp.float32
    return pl.pallas_call(
        invert_kernel,
        out_shape=jax.ShapeDtypeStruct((size, size), f32),
        scratch_shapes=[
            pltpu.VMEM((size, size), f32),
            pltpu.VMEM((size, size), f32),
            pltpu.VMEM((tile, tile), f32),
            pltpu.VMEM((tile, tile), f32),
            pltpu.VMEM((tile, 2 * tile), f32),
            pltpu.VMEM((tile, tile), f32),
        ],
        name="inverse_factor",
    )(dense)


def exchange(value, axis, bit):
    count = lax.axis_size(axis)
    other = lax.ppermute(value, axis, [(i, i ^ bit) for i in range(count)])
    upper = (lax.axis_index(axis) & bit) != 0
    return jnp.stack([jnp.where(upper, other, value), jnp.where(upper, value, other)])


def gather_cols(value):
    count = lax.axis_size("col")
    bits = []
    bit = count // 2
    while bit:
        value = exchange(value, "col", bit)
        bits.append(bit)
        bit //= 2
    depth = len(bits)
    shape = value.shape[depth:]
    value = jnp.transpose(value, tuple(range(depth))[::-1] + tuple(range(depth, value.ndim)))
    return value.reshape((count,) + shape)


def gather_band(value, base):
    count = lax.axis_size("row")
    home = base // PT
    group = lax.axis_index("row") // PT
    value = jnp.where(group == home, value, 0.0)
    have = [home]
    step = 1
    while step < count // PT:
        pairs = []
        for g in have:
            pairs += [(g * PT + t, (g ^ step) * PT + t) for t in range(PT)]
        value = value + lax.ppermute(value, "row", pairs)
        have += [g ^ step for g in have]
        step *= 2
    depth = 0
    bit = PT // 2
    while bit:
        value = exchange(value, "row", bit)
        depth += 1
        bit //= 2
    shape = value.shape[depth:]
    value = jnp.transpose(value, tuple(range(depth))[::-1] + tuple(range(depth, value.ndim)))
    return value.reshape((PT,) + shape)


def mirror(dense):
    return jnp.tril(dense) + jnp.tril(dense, -1).T


def unpack(message, tile_rows, slots, tile):
    lead = message.shape[:-3]
    cols = message.shape[-3]
    n = len(lead)
    body = message[..., : tile_rows * slots * tile, :]
    body = body.reshape(lead + (cols, tile_rows, slots, tile, tile))
    order = tuple(range(n)) + (n + 1, n + 3, n + 2, n, n + 4)
    body = body.transpose(order).reshape(lead + (tile_rows, tile, slots * cols * tile))
    marks = message[..., tile_rows * slots * tile :, :][..., :tile_rows, :slots]
    order = tuple(range(n)) + (n + 1, n + 2, n)
    marks = marks.transpose(order).reshape(lead + (tile_rows, slots * cols))
    return body, marks


def on_device(matrix, flags):
    row_count = lax.axis_size("row")
    col_count = lax.axis_size("col")
    row_index = lax.axis_index("row")
    col_index = lax.axis_index("col")
    tile_rows = matrix.shape[0]
    tile_cols = matrix.shape[2]
    tile = matrix.shape[4]
    panel = PT * tile
    slots = PT * STEPS // col_count
    first = max(1, PT // col_count)
    fold = row_count // col_count
    tiles = matrix.reshape(tile_rows, tile_cols, tile, tile)
    marks = flags.reshape(tile_rows, tile_cols)
    row_ids = jnp.arange(tile_rows, dtype=jnp.int32) * row_count + row_index
    col_ids = jnp.arange(tile_cols, dtype=jnp.int32) * col_count + col_index
    work = jnp.where((marks == 1)[:, :, None, None], storage_round(tiles), tiles)
    own = work[:, :slots]
    own_marks = marks[:, :slots].astype(jnp.float32)

    def message(low, high):
        body = own[low:high].reshape(-1, tile)
        extra = jnp.pad(own_marks[low:high], ((0, PAD - (high - low)), (0, tile - slots)))
        return jnp.concatenate([body, extra], axis=0)

    skip = (PT * STEPS) // row_count
    pairs = []
    for r in range(row_count):
        for c in range(col_count):
            target = (r // col_count) * col_count + c
            pairs.append((r * col_count + c, target * col_count + r % col_count))
    spread = lax.ppermute(message(skip, tile_rows), ("row", "col"), pairs)
    right_all = lax.all_gather(spread, "row", axis=0)

    near = gather_cols(gather_band(own[0, :first], 0))
    near = near.transpose(1, 3, 2, 0, 4).reshape(panel, first * col_count * tile)[:, :panel]
    dense0 = mirror(near)
    inv0 = inverse_factor(dense0, tile)

    band = gather_cols(gather_band(message(0, 1), PT))
    band, band_marks = unpack(band.transpose(1, 0, 2, 3), 1, slots, tile)
    band = band.reshape(panel, STEPS * panel)
    band_marks = band_marks.reshape(PT, STEPS * PT)[:, PT:]
    solved_band = exact_dot(band[:, :panel], inv0, 1, 1)

    def reduce_rows(solved, rest, rest_marks):
        exact = exact_dot(solved, solved_band, 1, 1)
        coarse = coarse_dot(solved, solved_band, 1, 1)
        count = rest_marks.shape[0]
        pick = (rest_marks == 1.0)[:, None, :, None]
        shape = (count, tile, PT, tile)
        update = jnp.where(pick, coarse.reshape(shape), exact.reshape(shape))
        return rest - update.reshape(count * tile, panel)

    dense1 = mirror(reduce_rows(solved_band, band[:, panel:], band_marks))
    inv1 = inverse_factor(dense1, tile)

    left, left_marks = unpack(gather_cols(message(0, tile_rows)), tile_rows, slots, tile)

    def own_block(rows, dense, start):
        at = jnp.clip(row_index - start, 0, PT - 1)
        block = lax.dynamic_slice_in_dim(dense, at * tile, tile, axis=0)
        inside = (row_index >= start) & (row_index < start + PT)
        top = jnp.where(inside, block, rows[:tile])
        return jnp.concatenate([top, rows[tile:]], axis=0)

    left = left.reshape(tile_rows * tile, STEPS * panel)
    left0 = exact_dot(own_block(left[:, :panel], dense0, 0), inv0, 1, 1)
    rest = reduce_rows(left0, left[:, panel:], left_marks[:, PT:])
    left1 = exact_dot(own_block(rest, dense1, PT), inv1, 1, 1)
    left_all = jnp.concatenate([left0, left1], axis=1).reshape(tile_rows, tile, STEPS * panel)

    right_all = right_all.reshape((fold, col_count) + right_all.shape[1:])
    right, right_marks = unpack(right_all, tile_rows - skip, slots, tile)
    count = fold * (tile_rows - skip)
    right = right.swapaxes(0, 1).reshape(count, tile, STEPS * panel)[count - (tile_cols - slots) :]
    right_marks = right_marks.swapaxes(0, 1).reshape(count, STEPS * PT)
    right_marks = right_marks[count - (tile_cols - slots) :]
    count = tile_cols - slots
    right = right.reshape(count * tile, STEPS * panel)
    right0 = exact_dot(right[:, :panel], inv0, 1, 1)
    rest = reduce_rows(right0, right[:, panel:], right_marks[:, PT:])
    right1 = exact_dot(rest, inv1, 1, 1)
    right_all = jnp.concatenate([right0, right1], axis=1).reshape(count, tile, STEPS * panel)

    exact = jnp.einsum("aik,cjk->acij", left_all, right_all, precision=HIGHEST)
    coarse = jnp.einsum(
        "aik,cjk->acij",
        left_all.astype(jnp.bfloat16),
        right_all.astype(jnp.bfloat16),
        preferred_element_type=jnp.float32,
    )
    pick = (marks[:, slots:] == 1)[:, :, None, None]
    trailing = work[:, slots:] - jnp.where(pick, coarse, exact)

    mine = left_all.reshape(tile_rows, tile, slots, col_count, tile)
    mine = lax.dynamic_index_in_dim(mine, col_index, 3, keepdims=False).transpose(0, 2, 1, 3)
    lower = jnp.tril(jnp.ones((tile, tile), jnp.bool_))
    on_diagonal = (row_ids[:, None] == col_ids[None, :slots])[:, :, None, None]
    mine = jnp.where(on_diagonal & ~lower, 0.0, mine)

    final = jnp.concatenate([mine, trailing], axis=1)
    final = jnp.where((marks == 1)[:, :, None, None], storage_round(final), final)
    upper = row_ids[:, None] < col_ids[None, :]
    final = jnp.where(upper[:, :, None, None], jnp.float32(0.0), final)
    return final.reshape(matrix.shape)


def solution(mesh):
    return jax.shard_map(
        on_device,
        mesh=mesh,
        in_specs=(P(None, "row", None, "col", None, None), P(None, "row", None, "col")),
        out_specs=P(None, "row", None, "col", None, None),
        check_vma=False,
    )
```

```python
import functools

import jax
import jax.numpy as jnp
from jax import lax
from jax.experimental import pallas as pl
from jax.experimental.pallas import tpu as pltpu
from jax.sharding import PartitionSpec as P

PT = 4
STEPS = 2
PAD = 8
WIDTH = 16
MAX_ROWS = 1024
HIGHEST = lax.Precision.HIGHEST


def storage_round(values):
    narrow = lax.optimization_barrier(values.astype(jnp.bfloat16))
    return narrow.astype(jnp.float32)


def kernel_round(values):
    return values.astype(jnp.bfloat16).astype(jnp.float32)


def exact_dot(left, right, left_dim=1, right_dim=0):
    return lax.dot_general(
        left,
        right,
        (((left_dim,), (right_dim,)), ((), ())),
        precision=HIGHEST,
        preferred_element_type=jnp.float32,
    )


def split(values):
    first = values.astype(jnp.bfloat16)
    rest = values - first.astype(jnp.float32)
    second = rest.astype(jnp.bfloat16)
    third = (rest - second.astype(jnp.float32)).astype(jnp.bfloat16)
    return first, second, third


def store_split(ref, values):
    for n, part in enumerate(split(values)):
        ref[n] = part


def load_split(ref):
    return [ref[n] for n in range(3)]


def narrow_dot(left, right):
    return lax.dot_general(
        left, right, (((1,), (1,)), ((), ())), preferred_element_type=jnp.float32
    )


def split_dot(left, right):
    coarse = narrow_dot(left[0], right[0])
    small = narrow_dot(left[0], right[2]) + narrow_dot(left[2], right[0])
    small = small + narrow_dot(left[1], right[1])
    cross = narrow_dot(left[0], right[1]) + narrow_dot(left[1], right[0])
    return coarse, coarse + (cross + small)


def lower_solve(rows, inverse):
    half = inverse[0].shape[0] // 2
    low = split_dot([r[:, :half] for r in rows], [m[:half, :half] for m in inverse])[1]
    high = split_dot(rows, [m[half:, :] for m in inverse])[1]
    return jnp.concatenate([low, high], axis=1)


def lane_columns(rows, low):
    return [jnp.broadcast_to(rows[:, low + j : low + j + 1], rows.shape) for j in range(WIDTH)]


def weighted(weights, rows):
    terms = [weights[k] * rows[k : k + 1, :] for k in range(WIDTH)]
    while len(terms) > 1:
        terms = [a + b for a, b in zip(terms[::2], terms[1::2])]
    return terms[0]


def invert_tile(a_ref, b_ref, q_ref, out_ref):
    tile = a_ref.shape[0]
    ids = lax.broadcasted_iota(jnp.int32, (WIDTH, tile), 0)
    row_ids = lax.broadcasted_iota(jnp.int32, (tile, tile), 0)
    lane_ids = lax.broadcasted_iota(jnp.int32, (tile, tile), 1)
    b_ref[...] = (row_ids == lane_ids).astype(jnp.float32)
    q_ref[...] = jnp.zeros(q_ref.shape, jnp.float32)
    rows = a_ref[:WIDTH, :]
    extra = b_ref[:WIDTH, :]
    for low in range(0, tile, WIDTH):
        high = low + WIDTH
        columns = lane_columns(rows, low)
        if high < tile:
            ahead = a_ref[high : high + WIDTH, :]
            ahead_extra = b_ref[high : high + WIDTH, :]
            weights = lane_columns(ahead, low)
        scale = jnp.zeros((WIDTH, tile), jnp.float32)
        for k in range(WIDTH):
            root = lax.rsqrt(columns[k][k : k + 1, :])
            inverse = root * root
            pivot_extra = extra[k : k + 1, :]
            out_ref[low + k : low + k + 1, :] = pivot_extra * root
            factor = jnp.where(ids == k, 0.0, columns[k] * inverse)
            for j in range(k + 1, WIDTH):
                columns[j] = columns[j] - factor * columns[j][k : k + 1, :]
            rows = rows - factor * rows[k : k + 1, :]
            extra = extra - factor * pivot_extra
            scale = jnp.where(ids == k, inverse, scale)
        if high < tile:
            rows = rows * scale
            extra = extra * scale
            if high + WIDTH < tile:
                q_ref[low:high, :tile] = rows
                q_ref[low:high, tile:] = extra
                below = a_ref[high + WIDTH :, :]
                update = exact_dot(below, q_ref[...])
                a_ref[high + WIDTH :, :] = below - update[:, :tile]
                b_ref[high + WIDTH :, :] = b_ref[high + WIDTH :, :] - update[:, tile:]
                q_ref[low:high, :] = jnp.zeros((WIDTH, 2 * tile), jnp.float32)
            rows = ahead - weighted(weights, rows)
            extra = ahead_extra - weighted(weights, extra)


def invert_dense(work, extra, out_ref, a_ref, b_ref, q_ref, l_ref):
    tile = a_ref.shape[0]
    size = work.shape[0]
    extra[...] = jnp.zeros(extra.shape, jnp.float32)
    out_ref[...] = jnp.zeros(out_ref.shape, jnp.float32)
    for low in range(0, size, tile):
        high = low + tile
        a_ref[...] = work[low:high, low:high]
        invert_tile(a_ref, b_ref, q_ref, l_ref)
        lower = l_ref[...]
        out_ref[low:high, low:high] = lower
        if low:
            out_ref[low:high, :low] = exact_dot(lower, extra[low:high, :low])
        if high < size:
            inverse = exact_dot(lower, lower, 0, 0)
            below = work[high:, low:high]
            work[high:, high:] = work[high:, high:] - exact_dot(
                below, exact_dot(inverse, work[low:high, high:])
            )
            if low:
                extra[high:, :low] = extra[high:, :low] - exact_dot(
                    below, exact_dot(inverse, extra[low:high, :low])
                )
            extra[high:, low:high] = -exact_dot(below, inverse)


def mirror_tile(values):
    tile = values.shape[0]
    row_ids = lax.broadcasted_iota(jnp.int32, (tile, tile), 0)
    lane_ids = lax.broadcasted_iota(jnp.int32, (tile, tile), 1)
    return jnp.where(row_ids >= lane_ids, values, values.T)


def relative(step, count):
    mask = 0
    bit = 1
    half = count // 2
    while half:
        if step & half:
            mask |= bit
        bit *= 2
        half //= 2
    return mask


def store_mirrored(tiles, work, i, j, values):
    tile = values.shape[0]
    work[i * tile : (i + 1) * tile, j * tile : (j + 1) * tile] = values
    if i > j:
        work[j * tile : (j + 1) * tile, i * tile : (i + 1) * tile] = values.T


def first_kernel(place, *refs, col_count, slots):
    pieces = refs[:2]
    dense_ref, out_ref, tiles, inv, work, extra, a_ref, b_ref, q_ref, l_ref = refs[2:]
    tile = a_ref.shape[0]
    half = col_count // 2
    for step in range(col_count):
        column = place[1] ^ relative(step, col_count)
        for m in range(PT):
            row = (place[0] & (PT - 1)) ^ m
            for slot in range(slots):
                tiles[row, slot * col_count + column] = pieces[step // half][step % half, m, slot]
    for i in range(PT):
        for j in range(i + 1):
            values = tiles[i, j]
            store_mirrored(tiles, work, i, j, mirror_tile(values) if i == j else values)
    dense_ref[...] = work[...]
    invert_dense(work, extra, inv, a_ref, b_ref, q_ref, l_ref)
    store_split(out_ref, inv[...])


def second_kernel(place, inv_ref, *refs, col_count, slots):
    pieces = refs[:2]
    (dense_ref, out_ref, solved_ref, tiles, picks, inv, work, extra, a_ref, b_ref, q_ref, l_ref) = (
        refs[2:]
    )
    tile = a_ref.shape[0]
    half = col_count // 2
    for step in range(col_count):
        column = place[1] ^ relative(step, col_count)
        for m in range(PT):
            row = (place[0] & (PT - 1)) ^ m
            piece = pieces[step // half]
            for slot in range(slots):
                at = slot * col_count + column
                tiles[row, at] = piece[step % half, m, slot * tile : (slot + 1) * tile, :]
                mark = piece[step % half, m, slots * tile : slots * tile + 1, slot : slot + 1]
                picks[row, at] = jnp.broadcast_to(mark, (PAD, tile))
    for i in range(PT):
        for j in range(PT):
            work[i * tile : (i + 1) * tile, j * tile : (j + 1) * tile] = tiles[i, j]
    solved = lower_solve(split(work[...]), load_split(inv_ref))
    parts = split(solved)
    for n in range(3):
        solved_ref[n] = parts[n]
    coarse, exact = split_dot(parts, parts)
    for i in range(PT):
        for j in range(i + 1):
            at = (slice(i * tile, (i + 1) * tile), slice(j * tile, (j + 1) * tile))
            update = exact[at]
            if i != j:
                update = jnp.where(picks[i, PT + j][:1, :] == 1.0, coarse[at], update)
            values = tiles[i, PT + j] - update
            store_mirrored(tiles, work, i, j, mirror_tile(values) if i == j else values)
    dense_ref[...] = work[...]
    invert_dense(work, extra, inv, a_ref, b_ref, q_ref, l_ref)
    store_split(out_ref, inv[...])


def left_kernel(place, marks, inv0_ref, inv1_ref, band_ref, dense0_ref, dense1_ref, *refs, col_count, slots):
    pieces = refs[:col_count]
    parts_ref, mine_ref, tiles, picks, rows, rest = refs[col_count:]
    tile = mine_ref.shape[2]
    count = mine_ref.shape[0]
    panel = PT * tile
    for step in range(col_count):
        column = place[1] ^ relative(step, col_count)
        piece = pieces[step]
        for a in range(count):
            for slot in range(slots):
                at = slot * col_count + column
                low = (a * slots + slot) * tile
                tiles[a, at] = piece[low : low + tile, :]
                low = count * slots * tile + a
                picks[a, at] = jnp.broadcast_to(piece[low : low + 1, slot : slot + 1], (PAD, tile))
    inv0 = load_split(inv0_ref)
    inv1 = load_split(inv1_ref)
    band = load_split(band_ref)
    for a in range(count):
        for j in range(PT):
            rows[a * tile : (a + 1) * tile, j * tile : (j + 1) * tile] = tiles[a, j]

    @pl.when(place[0] < PT)
    def _():
        rows[:tile, :] = dense0_ref[pl.ds(pl.multiple_of(place[0] * tile, tile), tile), :]

    solved0 = lower_solve(split(rows[...]), inv0)
    coarse, exact = split_dot(split(solved0), band)
    for a in range(count):
        for j in range(PT):
            at = (slice(a * tile, (a + 1) * tile), slice(j * tile, (j + 1) * tile))
            pick = picks[a, PT + j][:1, :] == 1.0
            rest[at] = tiles[a, PT + j] - jnp.where(pick, coarse[at], exact[at])

    @pl.when((place[0] >= PT) & (place[0] < 2 * PT))
    def _():
        low = pl.multiple_of((place[0] - PT) * tile, tile)
        rest[:tile, :] = dense1_ref[pl.ds(low, tile), :]

    solved1 = lower_solve(split(rest[...]), inv1)
    for p, solved in enumerate((solved0, solved1)):
        for n, part in enumerate(split(solved)):
            parts_ref[n, :, p * panel : (p + 1) * panel] = part
        for a in range(count):
            for j in range(PT):
                tiles[a, p * PT + j] = solved[a * tile : (a + 1) * tile, j * tile : (j + 1) * tile]
    row_ids = lax.broadcasted_iota(jnp.int32, (tile, tile), 0)
    lane_ids = lax.broadcasted_iota(jnp.int32, (tile, tile), 1)
    for a in range(count):
        for slot in range(slots):
            i = a * place[2] + place[0]
            j = slot * col_count + place[1]
            values = tiles[a, j]
            values = jnp.where(marks[a, slot] == 1, kernel_round(values), values)
            mine_ref[a, slot] = jnp.where((i - j) * tile + row_ids >= lane_ids, values, 0.0)


def ring_place(row, count):
    return jnp.where(row % 2 == 0, row // 2, count - 1 - row // 2)


def ring_at(place, count):
    return jnp.where(place < count // 2, 2 * place, 2 * (count - 1 - place) + 1)


def final_kernel(place, marks, inv0_ref, inv1_ref, band_ref, parts_ref, mine_ref, work_ref, *refs, hops, col_count, slots, fold, skip):
    pieces = refs[: len(hops)]
    out_ref, tiles, picks, rows, right = refs[len(hops) :]
    tile = work_ref.shape[2]
    count = work_ref.shape[0]
    step = pl.program_id(0)
    panel = PT * tile
    held = count - skip
    group = fold * tile

    @pl.when(step == 0)
    def _():
        row_count = place[2]
        at = ring_place(place[0], row_count)
        for piece, hop in zip(pieces, hops):
            source = ring_at((at + row_count + hop) % row_count, row_count)
            g = source // col_count
            for a in range(held):
                for slot in range(slots):
                    column = slot * col_count + source % col_count
                    low = (a * slots + slot) * tile
                    tiles[a, g, column] = piece[low : low + tile, :]
                    low = held * slots * tile + a
                    mark = piece[low : low + 1, slot : slot + 1]
                    picks[a, g, column] = jnp.broadcast_to(mark, (PAD, tile))
        chunk = max(1, MAX_ROWS // group)
        for base in range(0, held, chunk):
            size = min(chunk, held - base) * group
            at = [
                (slice(n * tile, (n + 1) * tile), base + n // fold, n % fold)
                for n in range(size // tile)
            ]
            for span, a, g in at:
                for j in range(PT):
                    rows[span, j * tile : (j + 1) * tile] = tiles[a, g, j]
            out = slice(base * group, base * group + size)
            solved = lower_solve(split(rows[:size]), load_split(inv0_ref))
            parts0 = split(solved)
            for n in range(3):
                right[n, out, :panel] = parts0[n]
            coarse, exact = split_dot(parts0, load_split(band_ref))
            for span, a, g in at:
                for j in range(PT):
                    where = (span, slice(j * tile, (j + 1) * tile))
                    pick = picks[a, g, PT + j][:1, :] == 1.0
                    rows[where] = tiles[a, g, PT + j] - jnp.where(pick, coarse[where], exact[where])
            solved = lower_solve(split(rows[:size]), load_split(inv1_ref))
            for n, part in enumerate(split(solved)):
                right[n, out, panel:] = part

    for p in range(count):

        @pl.when(step == p)
        def _():
            if (p + 1) * fold > slots:
                low = max(p - skip, 0) * group
                other = [right[n, low : low + group, :] for n in range(3)]
                left = [parts_ref[n, p * tile :, :] for n in range(3)]
                coarse, exact = split_dot(left, other)
            for g in range(fold):
                q = p * fold + g
                j = q * col_count + place[1]
                for a in range(count):
                    i = a * place[2] + place[0]
                    if q < slots:
                        out_ref[a, g] = mine_ref[a, q]
                    elif a < p:
                        out_ref[a, g] = jnp.zeros((tile, tile), jnp.float32)
                    else:
                        where = (slice((a - p) * tile, (a - p + 1) * tile), slice(g * tile, (g + 1) * tile))
                        raw = work_ref[a, g]
                        flagged = marks[a, q] == 1
                        narrow = kernel_round(kernel_round(raw) - coarse[where])
                        values = jnp.where(flagged, narrow, raw - exact[where])
                        out_ref[a, g] = jnp.where(i >= j, values, 0.0)


SMEM = pl.BlockSpec(memory_space=pltpu.SMEM)
WHOLE = pl.BlockSpec(memory_space=pltpu.VMEM)


def factor_scratch(tile):
    f32 = jnp.float32
    size = PT * tile
    return [
        pltpu.VMEM((size, size), f32),
        pltpu.VMEM((size, size), f32),
        pltpu.VMEM((tile, tile), f32),
        pltpu.VMEM((tile, tile), f32),
        pltpu.VMEM((tile, 2 * tile), f32),
        pltpu.VMEM((tile, tile), f32),
    ]


def fetch(value, axis, bit):
    count = lax.axis_size(axis)
    return lax.ppermute(value, axis, [(i, i ^ bit) for i in range(count)])


def halve_cols(value):
    value = value[None]
    bit = lax.axis_size("col") // 2
    while bit > 1:
        value = jnp.concatenate([value, fetch(value, "col", bit)])
        bit //= 2
    return value


def last_cols(value):
    return [value, fetch(value, "col", 1)]


def spread_band(value, base):
    count = lax.axis_size("row")
    home = base // PT
    group = lax.axis_index("row") // PT
    have = [home]
    step = 1
    while step < count // PT:
        pairs = []
        for g in have:
            pairs += [(g * PT + t, (g ^ step) * PT + t) for t in range(PT)]
        moved = lax.ppermute(value, "row", pairs)
        value = jnp.where((group & step) == (home & step), value, moved)
        have += [g ^ step for g in have]
        step *= 2
    return value


def gather_band(value):
    return jnp.stack([value] + [fetch(value, "row", m) for m in range(1, PT)])


def cost(micros):
    return pl.CostEstimate(flops=int(micros * 250e6), bytes_accessed=0, transcendentals=0)


def on_device(matrix, flags):
    row_count = lax.axis_size("row")
    col_count = lax.axis_size("col")
    row_index = lax.axis_index("row")
    col_index = lax.axis_index("col")
    tile_rows = matrix.shape[0]
    tile_cols = matrix.shape[2]
    tile = matrix.shape[4]
    panel = PT * tile
    slots = PT * STEPS // col_count
    first = max(1, PT // col_count)
    fold = row_count // col_count
    skip = (PT * STEPS) // row_count
    f32 = jnp.float32
    bf16 = jnp.bfloat16
    tiles = matrix.reshape(tile_rows, tile_cols, tile, tile)
    marks = flags.reshape(tile_rows, tile_cols)
    place = jnp.stack([row_index, col_index, jnp.int32(row_count)]).astype(jnp.int32)
    own = tiles[:, :slots]
    own = jnp.where((marks[:, :slots] == 1)[:, :, None, None], storage_round(own), own)
    own_marks = marks[:, :slots].astype(f32)

    def message(low, high):
        body = own[low:high].reshape(-1, tile)
        extra = jnp.pad(own_marks[low:high], ((0, PAD - (high - low)), (0, tile - slots)))
        return jnp.concatenate([body, extra], axis=0)

    order = list(range(0, row_count, 2)) + list(range(1, row_count, 2))[::-1]
    forward = [(order[n], order[(n + 1) % row_count]) for n in range(row_count)]
    backward = [(b, a) for a, b in forward]

    pairs = []
    for r in range(row_count):
        for c in range(col_count):
            target = (r // col_count) * col_count + c
            pairs.append((r * col_count + c, target * col_count + r % col_count))

    share = lax.ppermute(message(skip, tile_rows), ("row", "col"), pairs)
    near = spread_band(own[0, :first], 0)
    band = spread_band(message(0, 1), PT)
    near, band = lax.optimization_barrier((near, band))
    near = gather_band(near)
    band = gather_band(band)
    near, band, share = lax.optimization_barrier((near, band, share))
    shares = {0: share}
    ahead = share
    behind = share

    def ring(step, ahead, behind):
        ahead = lax.ppermute(ahead, "row", forward)
        shares[-step] = ahead
        if 2 * step < row_count:
            behind = lax.ppermute(behind, "row", backward)
            shares[step] = behind
        return ahead, behind

    near = halve_cols(near)
    ahead, behind = ring(1, ahead, behind)
    near, band, mine = lax.optimization_barrier((near, band, message(0, tile_rows)))
    band = halve_cols(band)
    left = halve_cols(mine)
    near = last_cols(near)

    near, ahead, behind = lax.optimization_barrier((near, ahead, behind))
    shares[-1], shares[1] = ahead, behind
    total = row_count // 2
    splits = [2 + (total - 1) * n // 3 for n in range(4)]
    for step in range(splits[0], splits[1]):
        ahead, behind = ring(step, ahead, behind)
    dense0, inv0 = pl.pallas_call(
        functools.partial(first_kernel, col_count=col_count, slots=first),
        in_specs=[SMEM, WHOLE, WHOLE],
        out_shape=[
            jax.ShapeDtypeStruct((panel, panel), f32),
            jax.ShapeDtypeStruct((3, panel, panel), bf16),
        ],
        scratch_shapes=[
            pltpu.VMEM((PT, first * col_count, tile, tile), f32),
            pltpu.VMEM((panel, panel), f32),
        ]
        + factor_scratch(tile),
        cost_estimate=cost(20),
        name="first_block",
    )(place, *near)

    inv0, band, left, ahead, behind = lax.optimization_barrier((inv0, band, left, ahead, behind))
    band = last_cols(band)
    for step in range(splits[1], splits[2]):
        ahead, behind = ring(step, ahead, behind)
    dense1, inv1, solved_band = pl.pallas_call(
        functools.partial(second_kernel, col_count=col_count, slots=slots),
        in_specs=[SMEM] + [WHOLE] * 3,
        out_shape=[
            jax.ShapeDtypeStruct((panel, panel), f32),
            jax.ShapeDtypeStruct((3, panel, panel), bf16),
            jax.ShapeDtypeStruct((3, panel, panel), bf16),
        ],
        scratch_shapes=[
            pltpu.VMEM((PT, slots * col_count, tile, tile), f32),
            pltpu.VMEM((PT, slots * col_count, PAD, tile), f32),
            pltpu.VMEM((panel, panel), f32),
        ]
        + factor_scratch(tile),
        cost_estimate=cost(25),
        name="second_block",
    )(place, inv0, *band)

    left = last_cols(left)
    inv1, ahead, behind = lax.optimization_barrier((inv1, ahead, behind))
    for step in range(splits[2], splits[3]):
        ahead, behind = ring(step, ahead, behind)
    half = col_count // 2
    left = [left[n // half][n % half] for n in range(col_count)]
    parts, mine = pl.pallas_call(
        functools.partial(left_kernel, col_count=col_count, slots=slots),
        in_specs=[SMEM, SMEM] + [WHOLE] * (5 + col_count),
        out_shape=[
            jax.ShapeDtypeStruct((3, tile_rows * tile, STEPS * panel), bf16),
            jax.ShapeDtypeStruct((tile_rows, slots, tile, tile), f32),
        ],
        scratch_shapes=[
            pltpu.VMEM((tile_rows, slots * col_count, tile, tile), f32),
            pltpu.VMEM((tile_rows, slots * col_count, PAD, tile), f32),
            pltpu.VMEM((tile_rows * tile, panel), f32),
            pltpu.VMEM((tile_rows * tile, panel), f32),
        ],
        cost_estimate=cost(12),
        name="own_rows",
    )(place, marks, inv0, inv1, solved_band, dense0, dense1, *left)

    hops = sorted(shares)
    held = tile_rows - skip
    size = held * fold * tile
    block = pl.BlockSpec((tile_rows, fold, tile, tile), lambda s: (0, s, 0, 0))
    final = pl.pallas_call(
        functools.partial(
            final_kernel, hops=tuple(hops), col_count=col_count, slots=slots, fold=fold, skip=skip
        ),
        grid=(tile_rows,),
        in_specs=[SMEM, SMEM] + [WHOLE] * 5 + [block] + [WHOLE] * len(hops),
        out_specs=block,
        out_shape=jax.ShapeDtypeStruct((tile_rows, tile_cols, tile, tile), f32),
        scratch_shapes=[
            pltpu.VMEM((held, fold, slots * col_count, tile, tile), f32),
            pltpu.VMEM((held, fold, slots * col_count, PAD, tile), f32),
            pltpu.VMEM((max(fold * tile, min(size, MAX_ROWS)), panel), f32),
            pltpu.VMEM((3, size, STEPS * panel), bf16),
        ],
        cost_estimate=cost(20),
        name="trailing",
    )(place, marks, inv0, inv1, solved_band, parts, mine, tiles, *[shares[h] for h in hops])
    return final.reshape(matrix.shape)


def solution(mesh):
    return jax.shard_map(
        on_device,
        mesh=mesh,
        in_specs=(P(None, "row", None, "col", None, None), P(None, "row", None, "col")),
        out_specs=P(None, "row", None, "col", None, None),
        check_vma=False,
    )
```

```python
import functools

import jax
import jax.numpy as jnp
from jax import lax
from jax.experimental import pallas as pl
from jax.experimental.pallas import tpu as pltpu
from jax.sharding import PartitionSpec as P

PT = 4
STEPS = 2
PAD = 8
WIDTH = 16
DEPTH = 256
HIGHEST = lax.Precision.HIGHEST


def storage_round(values):
    narrow = lax.optimization_barrier(values.astype(jnp.bfloat16))
    return narrow.astype(jnp.float32)


def kernel_round(values):
    return values.astype(jnp.bfloat16).astype(jnp.float32)


def exact_dot(left, right, left_dim=1, right_dim=0):
    return lax.dot_general(
        left,
        right,
        (((left_dim,), (right_dim,)), ((), ())),
        precision=HIGHEST,
        preferred_element_type=jnp.float32,
    )


def split(values):
    first = values.astype(jnp.bfloat16)
    rest = values - first.astype(jnp.float32)
    second = rest.astype(jnp.bfloat16)
    third = (rest - second.astype(jnp.float32)).astype(jnp.bfloat16)
    return first, second, third


def store_split(ref, values):
    for n, part in enumerate(split(values)):
        ref[n] = part


def load_split(ref):
    return [ref[n] for n in range(3)]


def narrow_dot(left, right):
    return lax.dot_general(
        left, right, (((1,), (1,)), ((), ())), preferred_element_type=jnp.float32
    )


def split_dot(left, right):
    coarse = narrow_dot(left[0], right[0])
    small = narrow_dot(left[0], right[2]) + narrow_dot(left[2], right[0])
    small = small + narrow_dot(left[1], right[1])
    cross = narrow_dot(left[0], right[1]) + narrow_dot(left[1], right[0])
    return coarse, coarse + (cross + small)


def flat_dot(left, right):
    return lax.dot_general(
        left, right, (((1,), (0,)), ((), ())), preferred_element_type=jnp.float32
    )


def flat_split_dot(left, right):
    coarse = flat_dot(left[0], right[0])
    small = flat_dot(left[0], right[2]) + flat_dot(left[2], right[0])
    small = small + flat_dot(left[1], right[1])
    cross = flat_dot(left[0], right[1]) + flat_dot(left[1], right[0])
    return coarse, coarse + (cross + small)


def upper_solve(rows, inverse):
    half = inverse[0].shape[0] // 2
    low = flat_split_dot([r[:, :half] for r in rows], [m[:half, :half] for m in inverse])[1]
    high = flat_split_dot(rows, [m[:, half:] for m in inverse])[1]
    return jnp.concatenate([low, high], axis=1)


def lane_columns(rows, low):
    return [jnp.broadcast_to(rows[:, low + j : low + j + 1], rows.shape) for j in range(WIDTH)]


def weighted(weights, rows):
    terms = [weights[k] * rows[k : k + 1, :] for k in range(WIDTH)]
    while len(terms) > 1:
        terms = [a + b for a, b in zip(terms[::2], terms[1::2])]
    return terms[0]


def invert_tile(a_ref, b_ref, q_ref, out_ref):
    tile = a_ref.shape[0]
    ids = lax.broadcasted_iota(jnp.int32, (WIDTH, tile), 0)
    row_ids = lax.broadcasted_iota(jnp.int32, (tile, tile), 0)
    lane_ids = lax.broadcasted_iota(jnp.int32, (tile, tile), 1)
    b_ref[...] = (row_ids == lane_ids).astype(jnp.float32)
    q_ref[...] = jnp.zeros(q_ref.shape, jnp.float32)
    rows = a_ref[:WIDTH, :]
    extra = b_ref[:WIDTH, :]
    for low in range(0, tile, WIDTH):
        high = low + WIDTH
        columns = lane_columns(rows, low)
        if high < tile:
            ahead = a_ref[high : high + WIDTH, :]
            ahead_extra = b_ref[high : high + WIDTH, :]
            weights = lane_columns(ahead, low)
        scale = jnp.zeros((WIDTH, tile), jnp.float32)
        for k in range(WIDTH):
            root = lax.rsqrt(columns[k][k : k + 1, :])
            inverse = root * root
            pivot_extra = extra[k : k + 1, :]
            out_ref[low + k : low + k + 1, :] = pivot_extra * root
            factor = jnp.where(ids == k, 0.0, columns[k] * inverse)
            for j in range(k + 1, WIDTH):
                columns[j] = columns[j] - factor * columns[j][k : k + 1, :]
            rows = rows - factor * rows[k : k + 1, :]
            extra = extra - factor * pivot_extra
            scale = jnp.where(ids == k, inverse, scale)
        if high < tile:
            rows = rows * scale
            extra = extra * scale
            if high + WIDTH < tile:
                q_ref[low:high, :tile] = rows
                q_ref[low:high, tile:] = extra
                below = a_ref[high + WIDTH :, :]
                update = exact_dot(below, q_ref[...])
                a_ref[high + WIDTH :, :] = below - update[:, :tile]
                b_ref[high + WIDTH :, :] = b_ref[high + WIDTH :, :] - update[:, tile:]
                q_ref[low:high, :] = jnp.zeros((WIDTH, 2 * tile), jnp.float32)
            rows = ahead - weighted(weights, rows)
            extra = ahead_extra - weighted(weights, extra)


def lane_block(values, at, tile):
    out = values[:, :tile]
    for j in range(1, values.shape[1] // tile):
        out = jnp.where(at == j, values[:, j * tile : (j + 1) * tile], out)
    return out


def invert_dense(work, out_ref, a_ref, b_ref, q_ref, l_ref):
    count, tile, size = work.shape
    blocks = lax.broadcasted_iota(jnp.int32, (tile, size), 1) // tile

    def spread(values):
        return jnp.concatenate([values] * count, axis=1)

    def eliminate(k, _):
        rows = work[k]
        a_ref[...] = lane_block(rows, k, tile)
        invert_tile(a_ref, b_ref, q_ref, l_ref)
        lower = l_ref[...]
        inverse = exact_dot(lower, lower, 0, 0)
        done = jnp.where(blocks < k, exact_dot(lower, rows), 0.0)
        out_ref[pl.ds(pl.multiple_of(k * tile, tile), tile), :] = jnp.where(
            blocks == k, spread(lower), done
        )
        scaled = jnp.where(blocks == k, spread(inverse), exact_dot(inverse, rows))

        def reduce(i, _):
            below = work[i]
            update = exact_dot(lane_block(below, k, tile), scaled)
            work[i] = jnp.where(blocks == k, 0.0, below) - update
            return 0

        lax.fori_loop(k + 1, count, reduce, 0)
        return 0

    lax.fori_loop(0, count, eliminate, 0)


def mirror_tile(values):
    tile = values.shape[0]
    row_ids = lax.broadcasted_iota(jnp.int32, (tile, tile), 0)
    lane_ids = lax.broadcasted_iota(jnp.int32, (tile, tile), 1)
    return jnp.where(row_ids >= lane_ids, values, values.T)


def relative(step, count):
    mask = 0
    bit = 1
    half = count // 2
    while half:
        if step & half:
            mask |= bit
        bit *= 2
        half //= 2
    return mask


def store_mirrored(work, i, j, values):
    tile = values.shape[0]
    work[i, :, j * tile : (j + 1) * tile] = values
    if i > j:
        work[j, :, i * tile : (i + 1) * tile] = values.T


def store_chunks(ref, parts, lane, row, count):
    at = pl.ds(pl.multiple_of(row, count), count)
    for n, part in enumerate(parts):
        for c in range(part.shape[1] // DEPTH):
            ref[lane // DEPTH + c, n, at, :] = part[:, c * DEPTH : (c + 1) * DEPTH]


def first_kernel(place, *refs, col_count, slots):
    pieces = refs[:2]
    top_ref, out_ref, tiles, inv, work, a_ref, b_ref, q_ref, l_ref = refs[2:]
    tile = a_ref.shape[0]
    half = col_count // 2
    for step in range(col_count):
        column = place[1] ^ relative(step, col_count)
        for m in range(PT):
            row = (place[0] & (PT - 1)) ^ m
            for slot in range(slots):
                tiles[row, slot * col_count + column] = pieces[step // half][step % half, m, slot]
    for i in range(PT):
        for j in range(i + 1):
            values = tiles[i, j]
            store_mirrored(work, i, j, mirror_tile(values) if i == j else values)
    top_ref[...] = work[jnp.clip(place[0], 0, PT - 1)]
    invert_dense(work, inv, a_ref, b_ref, q_ref, l_ref)
    store_split(out_ref, inv[...].T)


def second_kernel(place, marks, inv_ref, top_ref, *refs, col_count, slots):
    pieces = refs[:2]
    lefts = refs[2 : 2 + col_count]
    out_ref, solved_ref, parts_ref, mine_ref = refs[2 + col_count : 6 + col_count]
    tiles, picks, owned, own_picks, rows, top1, inv, block, work, a_ref, b_ref, q_ref, l_ref = refs[
        6 + col_count :
    ]
    tile = a_ref.shape[0]
    panel = PT * tile
    count = mine_ref.shape[0]
    half = col_count // 2
    for step in range(col_count):
        column = place[1] ^ relative(step, col_count)
        for m in range(PT):
            row = (place[0] & (PT - 1)) ^ m
            piece = pieces[step // half]
            for slot in range(slots):
                at = slot * col_count + column
                tiles[row, at] = piece[step % half, m, slot * tile : (slot + 1) * tile, :]
                mark = piece[step % half, m, slots * tile : slots * tile + 1, slot : slot + 1]
                picks[row, at] = jnp.broadcast_to(mark, (PAD, tile))
        piece = lefts[step]
        for a in range(count):
            for slot in range(slots):
                at = slot * col_count + column
                low = (a * slots + slot) * tile
                owned[a, at] = piece[low : low + tile, :]
                low = count * slots * tile + a
                mark = piece[low : low + 1, slot : slot + 1]
                own_picks[a, at] = jnp.broadcast_to(mark, (PAD, tile))
    for i in range(PT):
        for j in range(PT):
            block[i * tile : (i + 1) * tile, j * tile : (j + 1) * tile] = tiles[i, j]
    solved = upper_solve(split(block[...]), load_split(inv_ref))
    band = split(solved)
    store_split(solved_ref, solved.T)
    coarse, exact = split_dot(band, band)
    for i in range(PT):
        for j in range(i + 1):
            at = (slice(i * tile, (i + 1) * tile), slice(j * tile, (j + 1) * tile))
            update = exact[at]
            if i != j:
                update = jnp.where(picks[i, PT + j][:1, :] == 1.0, coarse[at], update)
            values = tiles[i, PT + j] - update
            store_mirrored(work, i, j, mirror_tile(values) if i == j else values)
    top1[...] = work[jnp.clip(place[0] - PT, 0, PT - 1)]
    invert_dense(work, inv, a_ref, b_ref, q_ref, l_ref)
    store_split(out_ref, inv[...].T)

    def solve_own(a, _):
        inside0 = (a == 0) & (place[0] < PT)
        inside1 = (a == 0) & (place[0] >= PT) & (place[0] < 2 * PT)
        for j in range(PT):
            at = slice(j * tile, (j + 1) * tile)
            rows[:, at] = jnp.where(inside0, top_ref[:, at], owned[a, j])
        solved = upper_solve(split(rows[...]), load_split(inv_ref))
        parts = split(solved)
        store_chunks(parts_ref, parts, 0, a * tile, tile)
        coarse, exact = flat_split_dot(parts, load_split(solved_ref))
        for j in range(PT):
            at = slice(j * tile, (j + 1) * tile)
            owned[a, j] = solved[:, at]
            pick = own_picks[a, PT + j][:1, :] == 1.0
            values = owned[a, PT + j] - jnp.where(pick, coarse[:, at], exact[:, at])
            rows[:, at] = jnp.where(inside1, top1[:, at], values)
        solved = upper_solve(split(rows[...]), load_split(out_ref))
        store_chunks(parts_ref, split(solved), panel, a * tile, tile)
        for j in range(PT):
            owned[a, PT + j] = solved[:, j * tile : (j + 1) * tile]
        return 0

    lax.fori_loop(0, count, solve_own, 0)
    row_ids = lax.broadcasted_iota(jnp.int32, (tile, tile), 0)
    lane_ids = lax.broadcasted_iota(jnp.int32, (tile, tile), 1)
    for a in range(count):
        for slot in range(slots):
            i = a * place[2] + place[0]
            j = slot * col_count + place[1]
            values = owned[a, j]
            values = jnp.where(marks[a, slot] == 1, kernel_round(values), values)
            mine_ref[a, slot] = jnp.where((i - j) * tile + row_ids >= lane_ids, values, 0.0)


def ring_place(row, count):
    return jnp.where(row % 2 == 0, row // 2, count - 1 - row // 2)


def ring_at(place, count):
    return jnp.where(place < count // 2, 2 * place, 2 * (count - 1 - place) + 1)


def final_kernel(place, marks, inv0_ref, inv1_ref, band_ref, parts_ref, mine_ref, work_ref, *refs, hops, col_count, slots, fold, skip):
    pieces = refs[: len(hops)]
    (out_ref, tiles, picks, rows, right, near, far, inv0, inv1, band, parts, mine, sems) = refs[
        len(hops) :
    ]
    copies = [
        pltpu.make_async_copy(source, target, sems.at[n])
        for n, (source, target) in enumerate(
            ((inv0_ref, inv0), (band_ref, band), (inv1_ref, inv1), (mine_ref, mine), (parts_ref, parts))
        )
    ]
    tile = work_ref.shape[2]
    count = work_ref.shape[0]
    step = pl.program_id(0)
    panel = PT * tile
    held = count - skip
    group = fold * tile

    @pl.when(step == 0)
    def _():
        for copy in copies:
            copy.start()
        row_count = place[2]
        at = ring_place(place[0], row_count)
        for piece, hop in zip(pieces, hops):
            source = ring_at((at + row_count + hop) % row_count, row_count)
            g = source // col_count
            for a in range(held):
                for slot in range(slots):
                    column = slot * col_count + source % col_count
                    low = (a * slots + slot) * tile
                    tiles[a, g, column] = piece[low : low + tile, :]
                    low = held * slots * tile + a
                    mark = piece[low : low + 1, slot : slot + 1]
                    picks[a, g, column] = jnp.broadcast_to(mark, (PAD, tile))
        for copy in copies[:3]:
            copy.wait()

        def solve(a, _):
            for g in range(fold):
                for j in range(PT):
                    where = (slice(g * tile, (g + 1) * tile), slice(j * tile, (j + 1) * tile))
                    rows[where] = tiles[a, g, j]
            parts0 = split(upper_solve(split(rows[...]), load_split(inv0)))
            store_chunks(right, parts0, 0, a * group, group)
            coarse, exact = flat_split_dot(parts0, load_split(band))
            for g in range(fold):
                for j in range(PT):
                    where = (slice(g * tile, (g + 1) * tile), slice(j * tile, (j + 1) * tile))
                    pick = picks[a, g, PT + j][:1, :] == 1.0
                    rows[where] = tiles[a, g, PT + j] - jnp.where(pick, coarse[where], exact[where])
            solved = upper_solve(split(rows[...]), load_split(inv1))
            store_chunks(right, split(solved), panel, a * group, group)
            return 0

        lax.fori_loop(0, held, solve, 0)
        copies[3].wait()
        copies[4].wait()

    for p in range(count):

        @pl.when(step == p)
        def _():
            if (p + 1) * fold > slots:
                low = max(p - skip, 0) * group
                above = p * tile
                near[above:, :] = jnp.zeros((count * tile - above, group), jnp.float32)
                far[above:, :] = jnp.zeros((count * tile - above, group), jnp.float32)

                def accumulate(c, _):
                    other = [right[c, n, low : low + group, :] for n in range(3)]
                    left = [parts[c, n, above:, :] for n in range(3)]
                    coarse, exact = split_dot(left, other)
                    near[above:, :] += coarse
                    far[above:, :] += exact
                    return 0

                lax.fori_loop(0, STEPS * panel // DEPTH, accumulate, 0)
            for g in range(fold):
                q = p * fold + g
                j = q * col_count + place[1]
                for a in range(count):
                    i = a * place[2] + place[0]
                    if q < slots:
                        out_ref[a, g] = mine[a, q]
                    elif a < p:
                        out_ref[a, g] = jnp.zeros((tile, tile), jnp.float32)
                    else:
                        where = (slice(a * tile, (a + 1) * tile), slice(g * tile, (g + 1) * tile))
                        raw = work_ref[a, g]
                        flagged = marks[a, q] == 1
                        narrow = kernel_round(kernel_round(raw) - near[where])
                        values = jnp.where(flagged, narrow, raw - far[where])
                        out_ref[a, g] = jnp.where(i >= j, values, 0.0)


SMEM = pl.BlockSpec(memory_space=pltpu.SMEM)
WHOLE = pl.BlockSpec(memory_space=pltpu.VMEM)


def factor_scratch(tile):
    f32 = jnp.float32
    size = PT * tile
    return [
        pltpu.VMEM((PT, tile, size), f32),
        pltpu.VMEM((tile, tile), f32),
        pltpu.VMEM((tile, tile), f32),
        pltpu.VMEM((tile, 2 * tile), f32),
        pltpu.VMEM((tile, tile), f32),
    ]


def fetch(value, axis, bit):
    count = lax.axis_size(axis)
    return lax.ppermute(value, axis, [(i, i ^ bit) for i in range(count)])


def halve_cols(value):
    value = value[None]
    bit = lax.axis_size("col") // 2
    while bit > 1:
        value = jnp.concatenate([value, fetch(value, "col", bit)])
        bit //= 2
    return value


def last_cols(value):
    return [value, fetch(value, "col", 1)]


def spread_band(value, base):
    count = lax.axis_size("row")
    home = base // PT
    group = lax.axis_index("row") // PT
    have = [home]
    step = 1
    while step < count // PT:
        pairs = []
        for g in have:
            pairs += [(g * PT + t, (g ^ step) * PT + t) for t in range(PT)]
        moved = lax.ppermute(value, "row", pairs)
        value = jnp.where((group & step) == (home & step), value, moved)
        have += [g ^ step for g in have]
        step *= 2
    return value


def gather_band(value):
    return jnp.stack([value] + [fetch(value, "row", m) for m in range(1, PT)])


def cost(micros):
    return pl.CostEstimate(flops=int(micros * 250e6), bytes_accessed=0, transcendentals=0)


def on_device(matrix, flags):
    row_count = lax.axis_size("row")
    col_count = lax.axis_size("col")
    row_index = lax.axis_index("row")
    col_index = lax.axis_index("col")
    tile_rows = matrix.shape[0]
    tile_cols = matrix.shape[2]
    tile = matrix.shape[4]
    panel = PT * tile
    slots = PT * STEPS // col_count
    first = max(1, PT // col_count)
    fold = row_count // col_count
    skip = (PT * STEPS) // row_count
    f32 = jnp.float32
    bf16 = jnp.bfloat16
    tiles = matrix.reshape(tile_rows, tile_cols, tile, tile)
    marks = flags.reshape(tile_rows, tile_cols)
    place = jnp.stack([row_index, col_index, jnp.int32(row_count)]).astype(jnp.int32)
    own = tiles[:, :slots]
    own = jnp.where((marks[:, :slots] == 1)[:, :, None, None], storage_round(own), own)
    own_marks = marks[:, :slots].astype(f32)

    def message(low, high):
        body = own[low:high].reshape(-1, tile)
        extra = jnp.pad(own_marks[low:high], ((0, PAD - (high - low)), (0, tile - slots)))
        return jnp.concatenate([body, extra], axis=0)

    order = list(range(0, row_count, 2)) + list(range(1, row_count, 2))[::-1]
    forward = [(order[n], order[(n + 1) % row_count]) for n in range(row_count)]
    backward = [(b, a) for a, b in forward]

    pairs = []
    for r in range(row_count):
        for c in range(col_count):
            target = (r // col_count) * col_count + c
            pairs.append((r * col_count + c, target * col_count + r % col_count))

    share = lax.ppermute(message(skip, tile_rows), ("row", "col"), pairs)
    near = spread_band(own[0, :first], 0)
    band = spread_band(message(0, 1), PT)
    near, band = lax.optimization_barrier((near, band))
    near = gather_band(near)
    band = gather_band(band)
    near, band, share = lax.optimization_barrier((near, band, share))
    shares = {0: share}
    ahead = share
    behind = share

    def ring(step, ahead, behind):
        ahead = lax.ppermute(ahead, "row", forward)
        shares[-step] = ahead
        if 2 * step < row_count:
            behind = lax.ppermute(behind, "row", backward)
            shares[step] = behind
        return ahead, behind

    near = halve_cols(near)
    ahead, behind = ring(1, ahead, behind)
    near, band, mine = lax.optimization_barrier((near, band, message(0, tile_rows)))
    band = halve_cols(band)
    left = halve_cols(mine)
    near = last_cols(near)

    near, ahead, behind = lax.optimization_barrier((near, ahead, behind))
    shares[-1], shares[1] = ahead, behind
    total = row_count // 2
    middle = max(2, total // 2)
    for step in range(2, middle + 1):
        ahead, behind = ring(step, ahead, behind)
    top0, inv0 = pl.pallas_call(
        functools.partial(first_kernel, col_count=col_count, slots=first),
        in_specs=[SMEM, WHOLE, WHOLE],
        out_shape=[
            jax.ShapeDtypeStruct((tile, panel), f32),
            jax.ShapeDtypeStruct((3, panel, panel), bf16),
        ],
        scratch_shapes=[
            pltpu.VMEM((PT, first * col_count, tile, tile), f32),
            pltpu.VMEM((panel, panel), f32),
        ]
        + factor_scratch(tile),
        cost_estimate=cost(18),
        compiler_params=pltpu.CompilerParams(vmem_limit_bytes=20 * 2**20),
        name="first_block",
    )(place, *near)

    inv0, band, left, ahead, behind = lax.optimization_barrier((inv0, band, left, ahead, behind))
    band = last_cols(band)
    left = last_cols(left)
    for step in range(middle + 1, total - 1):
        ahead, behind = ring(step, ahead, behind)
    cut = share.shape[0] // 16 * 8
    double = [(order[n], order[(n + 2) % row_count]) for n in range(row_count)]
    across = [
        lax.ppermute(ahead[:cut], "row", double),
        lax.ppermute(behind[cut:], "row", [(b, a) for a, b in double]),
    ]
    ring(total - 1, ahead, behind)
    half = col_count // 2
    left = [left[n // half][n % half] for n in range(col_count)]
    inv1, solved_band, parts, mine = pl.pallas_call(
        functools.partial(second_kernel, col_count=col_count, slots=slots),
        in_specs=[SMEM, SMEM] + [WHOLE] * (4 + col_count),
        out_shape=[
            jax.ShapeDtypeStruct((3, panel, panel), bf16),
            jax.ShapeDtypeStruct((3, panel, panel), bf16),
            jax.ShapeDtypeStruct((STEPS * panel // DEPTH, 3, tile_rows * tile, DEPTH), bf16),
            jax.ShapeDtypeStruct((tile_rows, slots, tile, tile), f32),
        ],
        scratch_shapes=[
            pltpu.VMEM((PT, slots * col_count, tile, tile), f32),
            pltpu.VMEM((PT, slots * col_count, PAD, tile), f32),
            pltpu.VMEM((tile_rows, slots * col_count, tile, tile), f32),
            pltpu.VMEM((tile_rows, slots * col_count, PAD, tile), f32),
            pltpu.VMEM((tile, panel), f32),
            pltpu.VMEM((tile, panel), f32),
            pltpu.VMEM((panel, panel), f32),
            pltpu.VMEM((panel, panel), f32),
        ]
        + factor_scratch(tile),
        cost_estimate=cost(30),
        name="second_block",
    )(place, marks, inv0, top0, *band, *left)
    mine, across, shares = lax.optimization_barrier((mine, across, shares))
    shares[-total] = jnp.concatenate(across)

    hops = sorted(shares)
    held = tile_rows - skip
    size = held * fold * tile
    block = pl.BlockSpec((tile_rows, fold, tile, tile), lambda s: (0, s, 0, 0))
    final = pl.pallas_call(
        functools.partial(
            final_kernel, hops=tuple(hops), col_count=col_count, slots=slots, fold=fold, skip=skip
        ),
        grid=(tile_rows,),
        in_specs=[SMEM, SMEM]
        + [pl.BlockSpec(memory_space=pl.ANY)] * 5
        + [block]
        + [WHOLE] * len(hops),
        out_specs=block,
        out_shape=jax.ShapeDtypeStruct((tile_rows, tile_cols, tile, tile), f32),
        scratch_shapes=[
            pltpu.VMEM((held, fold, slots * col_count, tile, tile), f32),
            pltpu.VMEM((held, fold, slots * col_count, PAD, tile), f32),
            pltpu.VMEM((fold * tile, panel), f32),
            pltpu.VMEM((STEPS * panel // DEPTH, 3, size, DEPTH), bf16),
            pltpu.VMEM((tile_rows * tile, fold * tile), f32),
            pltpu.VMEM((tile_rows * tile, fold * tile), f32),
            pltpu.VMEM((3, panel, panel), bf16),
            pltpu.VMEM((3, panel, panel), bf16),
            pltpu.VMEM((3, panel, panel), bf16),
            pltpu.VMEM((STEPS * panel // DEPTH, 3, tile_rows * tile, DEPTH), bf16),
            pltpu.VMEM((tile_rows, slots, tile, tile), f32),
            pltpu.SemaphoreType.DMA((5,)),
        ],
        cost_estimate=cost(20),
        name="trailing",
    )(place, marks, inv0, inv1, solved_band, parts, mine, tiles, *[shares[h] for h in hops])
    return final.reshape(matrix.shape)


def solution(mesh):
    return jax.shard_map(
        on_device,
        mesh=mesh,
        in_specs=(P(None, "row", None, "col", None, None), P(None, "row", None, "col")),
        out_specs=P(None, "row", None, "col", None, None),
        check_vma=False,
    )
```

```python
import functools

import jax
import jax.numpy as jnp
from jax import lax
from jax.experimental import pallas as pl
from jax.experimental.pallas import tpu as pltpu
from jax.sharding import PartitionSpec as P

PT = 4
STEPS = 2
PAD = 8
WIDTH = 16
DEPTH = 256
HIGHEST = lax.Precision.HIGHEST


def storage_round(values):
    narrow = lax.optimization_barrier(values.astype(jnp.bfloat16))
    return narrow.astype(jnp.float32)


def kernel_round(values):
    return values.astype(jnp.bfloat16).astype(jnp.float32)


def exact_dot(left, right, left_dim=1, right_dim=0):
    return lax.dot_general(
        left,
        right,
        (((left_dim,), (right_dim,)), ((), ())),
        precision=HIGHEST,
        preferred_element_type=jnp.float32,
    )


def split(values):
    first = values.astype(jnp.bfloat16)
    rest = values - first.astype(jnp.float32)
    second = rest.astype(jnp.bfloat16)
    third = (rest - second.astype(jnp.float32)).astype(jnp.bfloat16)
    return first, second, third


def store_split(ref, values):
    for n, part in enumerate(split(values)):
        ref[n] = part


def load_split(ref):
    return [ref[n] for n in range(3)]


def narrow_dot(left, right):
    return lax.dot_general(
        left, right, (((1,), (1,)), ((), ())), preferred_element_type=jnp.float32
    )


def split_dot(left, right):
    coarse = narrow_dot(left[0], right[0])
    small = narrow_dot(left[0], right[2]) + narrow_dot(left[2], right[0])
    small = small + narrow_dot(left[1], right[1])
    cross = narrow_dot(left[0], right[1]) + narrow_dot(left[1], right[0])
    return coarse, coarse + (cross + small)


def flat_dot(left, right):
    return lax.dot_general(
        left, right, (((1,), (0,)), ((), ())), preferred_element_type=jnp.float32
    )


def flat_split_dot(left, right):
    coarse = flat_dot(left[0], right[0])
    small = flat_dot(left[0], right[2]) + flat_dot(left[2], right[0])
    small = small + flat_dot(left[1], right[1])
    cross = flat_dot(left[0], right[1]) + flat_dot(left[1], right[0])
    return coarse, coarse + (cross + small)


def upper_solve(rows, inverse):
    half = inverse[0].shape[0] // 2
    low = flat_split_dot([r[:, :half] for r in rows], [m[:half, :half] for m in inverse])[1]
    high = flat_split_dot(rows, [m[:, half:] for m in inverse])[1]
    return jnp.concatenate([low, high], axis=1)


def lane_columns(rows, low):
    return [jnp.broadcast_to(rows[:, low + j : low + j + 1], rows.shape) for j in range(WIDTH)]


def weighted(weights, rows):
    terms = [weights[k] * rows[k : k + 1, :] for k in range(WIDTH)]
    while len(terms) > 1:
        terms = [a + b for a, b in zip(terms[::2], terms[1::2])]
    return terms[0]


def invert_tile(a_ref, b_ref, q_ref, out_ref):
    tile = a_ref.shape[0]
    ids = lax.broadcasted_iota(jnp.int32, (WIDTH, tile), 0)
    row_ids = lax.broadcasted_iota(jnp.int32, (tile, tile), 0)
    lane_ids = lax.broadcasted_iota(jnp.int32, (tile, tile), 1)
    b_ref[...] = (row_ids == lane_ids).astype(jnp.float32)
    q_ref[...] = jnp.zeros(q_ref.shape, jnp.float32)
    rows = a_ref[:WIDTH, :]
    extra = b_ref[:WIDTH, :]
    for low in range(0, tile, WIDTH):
        high = low + WIDTH
        columns = lane_columns(rows, low)
        if high < tile:
            ahead = a_ref[high : high + WIDTH, :]
            ahead_extra = b_ref[high : high + WIDTH, :]
            weights = lane_columns(ahead, low)
        scale = jnp.zeros((WIDTH, tile), jnp.float32)
        for k in range(WIDTH):
            root = lax.rsqrt(columns[k][k : k + 1, :])
            inverse = root * root
            pivot_extra = extra[k : k + 1, :]
            out_ref[low + k : low + k + 1, :] = pivot_extra * root
            factor = jnp.where(ids == k, 0.0, columns[k] * inverse)
            for j in range(k + 1, WIDTH):
                columns[j] = columns[j] - factor * columns[j][k : k + 1, :]
            rows = rows - factor * rows[k : k + 1, :]
            extra = extra - factor * pivot_extra
            scale = jnp.where(ids == k, inverse, scale)
        if high < tile:
            rows = rows * scale
            extra = extra * scale
            if high + WIDTH < tile:
                q_ref[low:high, :tile] = rows
                q_ref[low:high, tile:] = extra
                below = a_ref[high + WIDTH :, :]
                update = exact_dot(below, q_ref[...])
                a_ref[high + WIDTH :, :] = below - update[:, :tile]
                b_ref[high + WIDTH :, :] = b_ref[high + WIDTH :, :] - update[:, tile:]
                q_ref[low:high, :] = jnp.zeros((WIDTH, 2 * tile), jnp.float32)
            rows = ahead - weighted(weights, rows)
            extra = ahead_extra - weighted(weights, extra)


def lane_block(values, at, tile):
    out = values[:, :tile]
    for j in range(1, values.shape[1] // tile):
        out = jnp.where(at == j, values[:, j * tile : (j + 1) * tile], out)
    return out


def invert_dense(work, out_ref, a_ref, b_ref, q_ref, l_ref, begin=0, end=PT):
    count, tile, size = work.shape
    blocks = lax.broadcasted_iota(jnp.int32, (tile, size), 1) // tile

    def spread(values):
        return jnp.concatenate([values] * count, axis=1)

    def eliminate(k, _):
        rows = work[k]
        a_ref[...] = lane_block(rows, k, tile)
        invert_tile(a_ref, b_ref, q_ref, l_ref)
        lower = l_ref[...]
        inverse = exact_dot(lower, lower, 0, 0)
        done = jnp.where(blocks < k, exact_dot(lower, rows), 0.0)
        out_ref[pl.ds(pl.multiple_of(k * tile, tile), tile), :] = jnp.where(
            blocks == k, spread(lower), done
        )
        scaled = jnp.where(blocks == k, spread(inverse), exact_dot(inverse, rows))

        def reduce(i, _):
            below = work[i]
            update = exact_dot(lane_block(below, k, tile), scaled)
            work[i] = jnp.where(blocks == k, 0.0, below) - update
            return 0

        lax.fori_loop(k + 1, count, reduce, 0)
        return 0

    lax.fori_loop(begin, end, eliminate, 0)


def mirror_tile(values):
    tile = values.shape[0]
    row_ids = lax.broadcasted_iota(jnp.int32, (tile, tile), 0)
    lane_ids = lax.broadcasted_iota(jnp.int32, (tile, tile), 1)
    return jnp.where(row_ids >= lane_ids, values, values.T)


def relative(step, count):
    mask = 0
    bit = 1
    half = count // 2
    while half:
        if step & half:
            mask |= bit
        bit *= 2
        half //= 2
    return mask


def store_mirrored(work, i, j, values):
    tile = values.shape[0]
    work[i, :, j * tile : (j + 1) * tile] = values
    if i > j:
        work[j, :, i * tile : (i + 1) * tile] = values.T


def store_chunks(ref, parts, lane, row, count):
    at = pl.ds(pl.multiple_of(row, count), count)
    for n, part in enumerate(parts):
        for c in range(part.shape[1] // DEPTH):
            ref[lane // DEPTH + c, n, at, :] = part[:, c * DEPTH : (c + 1) * DEPTH]


def first_kernel(place, *refs, col_count, slots):
    pieces = refs[:2]
    top_ref, inv, work, tiles, a_ref, b_ref, q_ref, l_ref = refs[2:]
    tile = a_ref.shape[0]
    half = col_count // 2
    for step in range(col_count):
        column = place[1] ^ relative(step, col_count)
        for m in range(PT):
            row = (place[0] & (PT - 1)) ^ m
            for slot in range(slots):
                tiles[row, slot * col_count + column] = pieces[step // half][step % half, m, slot]
    for i in range(PT):
        for j in range(i + 1):
            values = tiles[i, j]
            store_mirrored(work, i, j, mirror_tile(values) if i == j else values)
    top_ref[...] = work[jnp.clip(place[0], 0, PT - 1)]
    invert_dense(work, inv, a_ref, b_ref, q_ref, l_ref, 0, PT // 2)


def finish_kernel(inv_ref, work_ref, out_ref, inv, work, a_ref, b_ref, q_ref, l_ref):
    half = inv_ref.shape[0] // 2
    inv[:half, :] = inv_ref[:half, :]
    work[...] = work_ref[...]
    invert_dense(work, inv, a_ref, b_ref, q_ref, l_ref, PT // 2, PT)
    store_split(out_ref, inv[...].T)


def second_kernel(place, inv_ref, *refs, col_count, slots):
    pieces = refs[:2]
    top1, inv, work, solved_ref, tiles, picks, block, a_ref, b_ref, q_ref, l_ref = refs[2:]
    tile = a_ref.shape[0]
    half = col_count // 2
    for step in range(col_count):
        column = place[1] ^ relative(step, col_count)
        for m in range(PT):
            row = (place[0] & (PT - 1)) ^ m
            piece = pieces[step // half]
            for slot in range(slots):
                at = slot * col_count + column
                tiles[row, at] = piece[step % half, m, slot * tile : (slot + 1) * tile, :]
                mark = piece[step % half, m, slots * tile : slots * tile + 1, slot : slot + 1]
                picks[row, at] = jnp.broadcast_to(mark, (PAD, tile))
    for i in range(PT):
        for j in range(PT):
            block[i * tile : (i + 1) * tile, j * tile : (j + 1) * tile] = tiles[i, j]
    solved = upper_solve(split(block[...]), load_split(inv_ref))
    band = split(solved)
    store_split(solved_ref, solved.T)
    coarse, exact = split_dot(band, band)
    for i in range(PT):
        for j in range(i + 1):
            at = (slice(i * tile, (i + 1) * tile), slice(j * tile, (j + 1) * tile))
            update = exact[at]
            if i != j:
                update = jnp.where(picks[i, PT + j][:1, :] == 1.0, coarse[at], update)
            values = tiles[i, PT + j] - update
            store_mirrored(work, i, j, mirror_tile(values) if i == j else values)
    top1[...] = work[jnp.clip(place[0] - PT, 0, PT - 1)]
    invert_dense(work, inv, a_ref, b_ref, q_ref, l_ref, 0, PT // 2)


def own_kernel(place, marks, inv0_ref, top_ref, solved_ref, top1, inv_ref, work_ref, *refs, col_count, slots):
    lefts = refs[:col_count]
    out_ref, parts_ref, mine_ref, owned, own_picks, rows, inv, work, a_ref, b_ref, q_ref, l_ref = refs[
        col_count:
    ]
    tile = a_ref.shape[0]
    panel = PT * tile
    count = mine_ref.shape[0]
    for step in range(col_count):
        column = place[1] ^ relative(step, col_count)
        piece = lefts[step]
        for a in range(count):
            for slot in range(slots):
                at = slot * col_count + column
                low = (a * slots + slot) * tile
                owned[a, at] = piece[low : low + tile, :]
                low = count * slots * tile + a
                mark = piece[low : low + 1, slot : slot + 1]
                own_picks[a, at] = jnp.broadcast_to(mark, (PAD, tile))
    finish_kernel(inv_ref, work_ref, out_ref, inv, work, a_ref, b_ref, q_ref, l_ref)

    def solve_own(a, _):
        inside0 = (a == 0) & (place[0] < PT)
        inside1 = (a == 0) & (place[0] >= PT) & (place[0] < 2 * PT)
        for j in range(PT):
            at = slice(j * tile, (j + 1) * tile)
            rows[:, at] = jnp.where(inside0, top_ref[:, at], owned[a, j])
        solved = upper_solve(split(rows[...]), load_split(inv0_ref))
        parts = split(solved)
        store_chunks(parts_ref, parts, 0, a * tile, tile)
        coarse, exact = flat_split_dot(parts, load_split(solved_ref))
        for j in range(PT):
            at = slice(j * tile, (j + 1) * tile)
            owned[a, j] = solved[:, at]
            pick = own_picks[a, PT + j][:1, :] == 1.0
            values = owned[a, PT + j] - jnp.where(pick, coarse[:, at], exact[:, at])
            rows[:, at] = jnp.where(inside1, top1[:, at], values)
        solved = upper_solve(split(rows[...]), load_split(out_ref))
        store_chunks(parts_ref, split(solved), panel, a * tile, tile)
        for j in range(PT):
            owned[a, PT + j] = solved[:, j * tile : (j + 1) * tile]
        return 0

    lax.fori_loop(0, count, solve_own, 0)
    row_ids = lax.broadcasted_iota(jnp.int32, (tile, tile), 0)
    lane_ids = lax.broadcasted_iota(jnp.int32, (tile, tile), 1)
    for a in range(count):
        for slot in range(slots):
            i = a * place[2] + place[0]
            j = slot * col_count + place[1]
            values = owned[a, j]
            values = jnp.where(marks[a, slot] == 1, kernel_round(values), values)
            mine_ref[a, slot] = jnp.where((i - j) * tile + row_ids >= lane_ids, values, 0.0)


def ring_place(row, count):
    return jnp.where(row % 2 == 0, row // 2, count - 1 - row // 2)


def ring_at(place, count):
    return jnp.where(place < count // 2, 2 * place, 2 * (count - 1 - place) + 1)


def final_kernel(place, marks, inv0_ref, inv1_ref, band_ref, parts_ref, mine_ref, work_ref, *refs, hops, col_count, slots, fold, skip):
    pieces = refs[: len(hops)]
    (out_ref, tiles, picks, rows, right, near, far, inv0, inv1, band, parts, mine, sems) = refs[
        len(hops) :
    ]
    copies = [
        pltpu.make_async_copy(source, target, sems.at[n])
        for n, (source, target) in enumerate(
            ((inv0_ref, inv0), (band_ref, band), (inv1_ref, inv1), (mine_ref, mine), (parts_ref, parts))
        )
    ]
    tile = work_ref.shape[2]
    count = work_ref.shape[0]
    step = pl.program_id(0)
    panel = PT * tile
    held = count - skip
    group = fold * tile

    @pl.when(step == 0)
    def _():
        for copy in copies:
            copy.start()
        row_count = place[2]
        at = ring_place(place[0], row_count)
        for piece, hop in zip(pieces, hops):
            source = ring_at((at + row_count + hop) % row_count, row_count)
            g = source // col_count
            for a in range(held):
                for slot in range(slots):
                    column = slot * col_count + source % col_count
                    low = (a * slots + slot) * tile
                    tiles[a, g, column] = piece[low : low + tile, :]
                    low = held * slots * tile + a
                    mark = piece[low : low + 1, slot : slot + 1]
                    picks[a, g, column] = jnp.broadcast_to(mark, (PAD, tile))
        for copy in copies[:3]:
            copy.wait()

        def solve(a, _):
            for g in range(fold):
                for j in range(PT):
                    where = (slice(g * tile, (g + 1) * tile), slice(j * tile, (j + 1) * tile))
                    rows[where] = tiles[a, g, j]
            parts0 = split(upper_solve(split(rows[...]), load_split(inv0)))
            store_chunks(right, parts0, 0, a * group, group)
            coarse, exact = flat_split_dot(parts0, load_split(band))
            for g in range(fold):
                for j in range(PT):
                    where = (slice(g * tile, (g + 1) * tile), slice(j * tile, (j + 1) * tile))
                    pick = picks[a, g, PT + j][:1, :] == 1.0
                    rows[where] = tiles[a, g, PT + j] - jnp.where(pick, coarse[where], exact[where])
            solved = upper_solve(split(rows[...]), load_split(inv1))
            store_chunks(right, split(solved), panel, a * group, group)
            return 0

        lax.fori_loop(0, held, solve, 0)
        copies[3].wait()
        copies[4].wait()

    for p in range(count):

        @pl.when(step == p)
        def _():
            if (p + 1) * fold > slots:
                low = max(p - skip, 0) * group
                above = p * tile
                near[above:, :] = jnp.zeros((count * tile - above, group), jnp.float32)
                far[above:, :] = jnp.zeros((count * tile - above, group), jnp.float32)

                def accumulate(c, _):
                    other = [right[c, n, low : low + group, :] for n in range(3)]
                    left = [parts[c, n, above:, :] for n in range(3)]
                    coarse, exact = split_dot(left, other)
                    near[above:, :] += coarse
                    far[above:, :] += exact
                    return 0

                lax.fori_loop(0, STEPS * panel // DEPTH, accumulate, 0)
            for g in range(fold):
                q = p * fold + g
                j = q * col_count + place[1]
                for a in range(count):
                    i = a * place[2] + place[0]
                    if q < slots:
                        out_ref[a, g] = mine[a, q]
                    elif a < p:
                        out_ref[a, g] = jnp.zeros((tile, tile), jnp.float32)
                    else:
                        where = (slice(a * tile, (a + 1) * tile), slice(g * tile, (g + 1) * tile))
                        raw = work_ref[a, g]
                        flagged = marks[a, q] == 1
                        narrow = kernel_round(kernel_round(raw) - near[where])
                        values = jnp.where(flagged, narrow, raw - far[where])
                        out_ref[a, g] = jnp.where(i >= j, values, 0.0)


SMEM = pl.BlockSpec(memory_space=pltpu.SMEM)
WHOLE = pl.BlockSpec(memory_space=pltpu.VMEM)


def factor_scratch(tile):
    f32 = jnp.float32
    size = PT * tile
    return [
        pltpu.VMEM((PT, tile, size), f32),
        pltpu.VMEM((tile, tile), f32),
        pltpu.VMEM((tile, tile), f32),
        pltpu.VMEM((tile, 2 * tile), f32),
        pltpu.VMEM((tile, tile), f32),
    ]


def fetch(value, axis, bit):
    count = lax.axis_size(axis)
    return lax.ppermute(value, axis, [(i, i ^ bit) for i in range(count)])


def begin_cols(value):
    value = value[None]
    return value, fetch(value, "col", lax.axis_size("col") // 2)


def finish_cols(value, far):
    value = jnp.concatenate([value, far])
    bit = lax.axis_size("col") // 4
    while bit > 1:
        value = jnp.concatenate([value, fetch(value, "col", bit)])
        bit //= 2
    return [value, fetch(value, "col", 1)]


def spread_band(value, base):
    count = lax.axis_size("row")
    home = base // PT
    group = lax.axis_index("row") // PT
    have = [home]
    step = 1
    while step < count // PT:
        pairs = []
        for g in have:
            pairs += [(g * PT + t, (g ^ step) * PT + t) for t in range(PT)]
        moved = lax.ppermute(value, "row", pairs)
        value = jnp.where((group & step) == (home & step), value, moved)
        have += [g ^ step for g in have]
        step *= 2
    return value


def gather_band(value):
    return jnp.stack([value] + [fetch(value, "row", m) for m in range(1, PT)])


def cost(micros):
    return pl.CostEstimate(flops=int(micros * 250e6), bytes_accessed=0, transcendentals=0)


def on_device(matrix, flags):
    row_count = lax.axis_size("row")
    col_count = lax.axis_size("col")
    row_index = lax.axis_index("row")
    col_index = lax.axis_index("col")
    tile_rows = matrix.shape[0]
    tile_cols = matrix.shape[2]
    tile = matrix.shape[4]
    panel = PT * tile
    slots = PT * STEPS // col_count
    first = max(1, PT // col_count)
    fold = row_count // col_count
    skip = (PT * STEPS) // row_count
    f32 = jnp.float32
    bf16 = jnp.bfloat16
    tiles = matrix.reshape(tile_rows, tile_cols, tile, tile)
    marks = flags.reshape(tile_rows, tile_cols)
    place = jnp.stack([row_index, col_index, jnp.int32(row_count)]).astype(jnp.int32)
    own = tiles[:, :slots]
    own = jnp.where((marks[:, :slots] == 1)[:, :, None, None], storage_round(own), own)
    own_marks = marks[:, :slots].astype(f32)

    def message(low, high):
        body = own[low:high].reshape(-1, tile)
        extra = jnp.pad(own_marks[low:high], ((0, PAD - (high - low)), (0, tile - slots)))
        return jnp.concatenate([body, extra], axis=0)

    order = list(range(0, row_count, 2)) + list(range(1, row_count, 2))[::-1]
    forward = [(order[n], order[(n + 1) % row_count]) for n in range(row_count)]
    backward = [(b, a) for a, b in forward]

    pairs = []
    for r in range(row_count):
        for c in range(col_count):
            target = (r // col_count) * col_count + c
            pairs.append((r * col_count + c, target * col_count + r % col_count))

    near = spread_band(own[0, :first], 0)
    band = spread_band(message(0, 1), PT)
    near = gather_band(near)
    near, band = lax.optimization_barrier((near, band))
    near = begin_cols(near)
    band = gather_band(band)
    shares = {}

    def ring(step, ahead, behind):
        ahead = lax.ppermute(ahead, "row", forward)
        shares[-step] = ahead
        if 2 * step < row_count:
            behind = lax.ppermute(behind, "row", backward)
            shares[step] = behind
        return ahead, behind

    near, band = lax.optimization_barrier((near, band))
    band = begin_cols(band)
    near = finish_cols(*near)
    near, shared = lax.optimization_barrier((near, message(skip, tile_rows)))
    share = lax.ppermute(shared, ("row", "col"), pairs)
    total = row_count // 2
    top0, inv0, work0 = pl.pallas_call(
        functools.partial(first_kernel, col_count=col_count, slots=first),
        in_specs=[SMEM, WHOLE, WHOLE],
        out_shape=[
            jax.ShapeDtypeStruct((tile, panel), f32),
            jax.ShapeDtypeStruct((panel, panel), f32),
            jax.ShapeDtypeStruct((PT, tile, panel), f32),
        ],
        scratch_shapes=[pltpu.VMEM((PT, first * col_count, tile, tile), f32)]
        + factor_scratch(tile)[1:],
        cost_estimate=cost(9),
        compiler_params=pltpu.CompilerParams(vmem_limit_bytes=20 * 2**20),
        name="first_block",
    )(place, *near)

    inv0, work0, share, mine = lax.optimization_barrier(
        (inv0, work0, share, message(0, tile_rows))
    )
    left = begin_cols(mine)
    shares[0] = share
    ahead, behind = ring(1, share, share)
    inv0 = pl.pallas_call(
        finish_kernel,
        in_specs=[WHOLE, WHOLE],
        out_specs=WHOLE,
        out_shape=jax.ShapeDtypeStruct((3, panel, panel), bf16),
        scratch_shapes=[pltpu.VMEM((panel, panel), f32)] + factor_scratch(tile),
        cost_estimate=cost(9),
        compiler_params=pltpu.CompilerParams(vmem_limit_bytes=20 * 2**20),
        name="first_block_rest",
    )(inv0, work0)

    inv0, band, ahead, behind = lax.optimization_barrier((inv0, band, ahead, behind))
    shares[-1], shares[1] = ahead, behind
    band = finish_cols(*band)
    middle = max(2, total // 2)
    for step in range(2, middle + 1):
        ahead, behind = ring(step, ahead, behind)
    top1, inv1, work1, solved_band = pl.pallas_call(
        functools.partial(second_kernel, col_count=col_count, slots=slots),
        in_specs=[SMEM] + [WHOLE] * 3,
        out_shape=[
            jax.ShapeDtypeStruct((tile, panel), f32),
            jax.ShapeDtypeStruct((panel, panel), f32),
            jax.ShapeDtypeStruct((PT, tile, panel), f32),
            jax.ShapeDtypeStruct((3, panel, panel), bf16),
        ],
        scratch_shapes=[
            pltpu.VMEM((PT, slots * col_count, tile, tile), f32),
            pltpu.VMEM((PT, slots * col_count, PAD, tile), f32),
            pltpu.VMEM((panel, panel), f32),
        ]
        + factor_scratch(tile)[1:],
        cost_estimate=cost(16),
        compiler_params=pltpu.CompilerParams(vmem_limit_bytes=32 * 2**20),
        name="second_block",
    )(place, inv0, *band)

    inv1, work1, left, ahead, behind = lax.optimization_barrier((inv1, work1, left, ahead, behind))
    left = finish_cols(*left)
    shares[-middle], shares[middle] = ahead, behind
    for step in range(middle + 1, total - 1):
        ahead, behind = ring(step, ahead, behind)
    cut = share.shape[0] // 16 * 8
    double = [(order[n], order[(n + 2) % row_count]) for n in range(row_count)]
    across = [
        lax.ppermute(ahead[:cut], "row", double),
        lax.ppermute(behind[cut:], "row", [(b, a) for a, b in double]),
    ]
    ring(total - 1, ahead, behind)
    half = col_count // 2
    left = [left[n // half][n % half] for n in range(col_count)]
    inv1, parts, mine = pl.pallas_call(
        functools.partial(own_kernel, col_count=col_count, slots=slots),
        in_specs=[SMEM, SMEM] + [WHOLE] * (6 + col_count),
        out_shape=[
            jax.ShapeDtypeStruct((3, panel, panel), bf16),
            jax.ShapeDtypeStruct((STEPS * panel // DEPTH, 3, tile_rows * tile, DEPTH), bf16),
            jax.ShapeDtypeStruct((tile_rows, slots, tile, tile), f32),
        ],
        scratch_shapes=[
            pltpu.VMEM((tile_rows, slots * col_count, tile, tile), f32),
            pltpu.VMEM((tile_rows, slots * col_count, PAD, tile), f32),
            pltpu.VMEM((tile, panel), f32),
            pltpu.VMEM((panel, panel), f32),
        ]
        + factor_scratch(tile),
        cost_estimate=cost(24),
        compiler_params=pltpu.CompilerParams(vmem_limit_bytes=40 * 2**20),
        name="own_rows",
    )(place, marks, inv0, top0, solved_band, top1, inv1, work1, *left)
    mine, across, shares = lax.optimization_barrier((mine, across, shares))
    shares[-total] = jnp.concatenate(across)

    hops = sorted(shares)
    held = tile_rows - skip
    size = held * fold * tile
    room = 44 * 2**20 if size <= 1024 else None
    block = pl.BlockSpec((tile_rows, fold, tile, tile), lambda s: (0, s, 0, 0))
    final = pl.pallas_call(
        functools.partial(
            final_kernel, hops=tuple(hops), col_count=col_count, slots=slots, fold=fold, skip=skip
        ),
        grid=(tile_rows,),
        in_specs=[SMEM, SMEM]
        + [pl.BlockSpec(memory_space=pl.ANY)] * 5
        + [block]
        + [WHOLE] * len(hops),
        out_specs=block,
        out_shape=jax.ShapeDtypeStruct((tile_rows, tile_cols, tile, tile), f32),
        scratch_shapes=[
            pltpu.VMEM((held, fold, slots * col_count, tile, tile), f32),
            pltpu.VMEM((held, fold, slots * col_count, PAD, tile), f32),
            pltpu.VMEM((fold * tile, panel), f32),
            pltpu.VMEM((STEPS * panel // DEPTH, 3, size, DEPTH), bf16),
            pltpu.VMEM((tile_rows * tile, fold * tile), f32),
            pltpu.VMEM((tile_rows * tile, fold * tile), f32),
            pltpu.VMEM((3, panel, panel), bf16),
            pltpu.VMEM((3, panel, panel), bf16),
            pltpu.VMEM((3, panel, panel), bf16),
            pltpu.VMEM((STEPS * panel // DEPTH, 3, tile_rows * tile, DEPTH), bf16),
            pltpu.VMEM((tile_rows, slots, tile, tile), f32),
            pltpu.SemaphoreType.DMA((5,)),
        ],
        cost_estimate=cost(20),
        compiler_params=pltpu.CompilerParams(vmem_limit_bytes=room),
        name="trailing",
    )(place, marks, inv0, inv1, solved_band, parts, mine, tiles, *[shares[h] for h in hops])
    return final.reshape(matrix.shape)


def solution(mesh):
    return jax.shard_map(
        on_device,
        mesh=mesh,
        in_specs=(P(None, "row", None, "col", None, None), P(None, "row", None, "col")),
        out_specs=P(None, "row", None, "col", None, None),
        check_vma=False,
    )
```
